32 devices in a mesh: area: 8 (over z, y), tie: 4 (over x, core).
Axes of the slice: x: 2, y: 2, z: 4, core: 2. Of those that a mesh axis runs over, the one named last changes fastest.
Arguments:
- ginv: bfloat16 [128, 1024, 1024], P(('area', 'tie'))
- rhs: float32 [131072, 128], P(('area', 'tie')), may hold values from -6 to 6
- bnd_row: int32 [128, 128], P(('area', 'tie')), may hold values from -1 to 1023, as said below
- bnd_var: int32 [128, 128], P(('area', 'tie')), may hold values from -1 to 2047, as said below
Outputs:
- states: float32 [131072, 128], P(('area', 'tie'))
- consensus: float32 [2048, 128], P(('area', 'tie'))
- dual_value: float32 [16384, 128], P(('area', 'tie'))
The draws below stay inside these ranges and needn't reach their ends.
Inputs may be any that keep to these rules, and one draw needn't show every extreme that they name: `bnd_row`: -1 marks an unused entry slot; the live rows of one area are distinct. `bnd_var`: -1 exactly where bnd_row is -1. Variable v is owned by the device holding rows v of the consensus output, block v // 64. The areas of one device hold at most 4 live entries owned by any one device; in every draw some owner holds exactly 4 from every device.
All inputs are finite; a program needn't handle non-finite values.
Results may differ from the reference program's by a relative error of at most 0.003.
Values sent between devices are 32-bit elements; how exact they have to be, the bound alone decides.
A program may use at most 64 MiB of HBM per device.

```python
import jax
import jax.numpy as jnp
from jax import lax

STATE = 1024
BND = 128
SLOT = 4
VAR_DEV = 64
AREA_DEV = 4
SNAP = 128
ITERS = 4
AREAS = 128
VARS = 2048


def boundary_maps(key):
    device_total = AREAS // AREA_DEV
    entries = AREA_DEV * BND
    hottest = jax.random.randint(jax.random.fold_in(key, 11), (), 0, device_total)
    slot_counts = jax.random.randint(jax.random.fold_in(key, 12), (device_total, device_total), 1, SLOT + 1)
    owner_ids = jnp.arange(device_total, dtype=jnp.int32)
    slot_counts = jnp.where(owner_ids[None, :] == hottest, SLOT, slot_counts)
    slot_live = jnp.arange(SLOT)[None, None, :] < slot_counts[:, :, None]
    local_ids = jax.random.randint(jax.random.fold_in(key, 13), (device_total, device_total, SLOT), 0, VAR_DEV)
    var_slot = jnp.where(slot_live, owner_ids[None, :, None] * VAR_DEV + local_ids, -1)
    var_slot = var_slot.reshape(device_total, device_total * SLOT).astype(jnp.int32)
    perm_keys = jax.random.split(jax.random.fold_in(key, 14), device_total)
    placing = jax.vmap(lambda k: jax.random.permutation(k, entries))(perm_keys)[:, :device_total * SLOT]
    entry_var = jnp.full((device_total, entries), -1, jnp.int32)
    entry_var = entry_var.at[jnp.arange(device_total)[:, None], placing].set(var_slot)
    entry_var = entry_var.reshape(AREAS, BND)
    row_keys = jax.random.split(jax.random.fold_in(key, 15), AREAS)
    row_perm = jax.vmap(lambda k: jax.random.permutation(k, STATE))(row_keys)[:, :BND].astype(jnp.int32)
    entry_row = jnp.where(entry_var >= 0, row_perm, -1).astype(jnp.int32)
    return (entry_row, entry_var)


def draw_bnd_row(key, part):
    return boundary_maps(key)[0]


def draw_bnd_var(key, part):
    return boundary_maps(key)[1]


def draw_ginv(key, part):
    area_keys = jax.random.split(jax.random.fold_in(key, 21), AREAS)

    def one_block(block_key):
        diag_values = jax.random.uniform(jax.random.fold_in(block_key, 7), (STATE,), jnp.float32, 0.3, 0.85)
        noise = jax.random.normal(block_key, (STATE, STATE), jnp.float32)
        return (jnp.diag(diag_values) + 0.3 * noise / STATE ** 0.5).astype(jnp.bfloat16)
    return lax.map(one_block, area_keys)


def block_levels(key, dims, shards, smallest, top_value):
    def one(dim, blocks):
        heights = jax.random.uniform(jax.random.fold_in(jax.random.fold_in(key, 6), dim), (blocks,), jnp.float32, smallest / len(shards), top_value / len(shards))
        return jnp.repeat(jnp.exp(heights), dims[dim] // blocks).reshape((-1,) + (1,) * (len(dims) - dim - 1))

    loudness = one(*shards[0])
    for cut in shards[1:]:
        loudness = loudness * one(*cut)
    return loudness


def scatter_about(stream_key, dims, deviation, most, cuts=(), kind=jnp.bfloat16):
    values = jax.random.normal(stream_key, dims, jnp.float32) * deviation
    if len(cuts) > 0:
        values = block_levels(stream_key, dims, cuts, -0.22, 0.18) * values
    return jnp.clip(values, min=-most, max=most).astype(kind)


def setup_inputs(seed: int = 0) -> dict:
    seeds = jax.random.split(jax.random.key(seed), 5)
    return {
        "ginv": draw_ginv(jax.random.fold_in(seeds[4], 71), 0),
        "rhs": scatter_about(seeds[1], (AREAS * STATE, SNAP), 1.0, 6.0, ((0, 32),), jnp.float32),
        "bnd_row": draw_bnd_row(jax.random.fold_in(seeds[4], 71), 0),
        "bnd_var": draw_bnd_var(jax.random.fold_in(seeds[4], 71), 0),
    }


PENALTY = 1.0


def solve_area(pair):
    return jnp.dot(pair[0], pair[1], preferred_element_type=jnp.float32)


def reference(ginv, rhs, bnd_row, bnd_var):
    areas_total, state_size, _ = ginv.shape
    snap_count = rhs.shape[1]
    active = (bnd_row >= 0).reshape(-1)
    offsets = (jnp.arange(areas_total, dtype=jnp.int32) * state_size)[:, None]
    rows_flat = jnp.where(bnd_row >= 0, offsets + bnd_row, 0).reshape(-1).astype(jnp.int32)
    var_safe = jnp.where(bnd_var >= 0, bnd_var, 0).reshape(-1).astype(jnp.int32)
    counts = jax.ops.segment_sum(active.astype(jnp.float32), var_safe, num_segments=VARS)
    inverse = 1.0 / jnp.maximum(counts, 1.0)
    mask = active[:, None]
    n_entries = rows_flat.shape[0]
    dual_value = jnp.zeros((n_entries, snap_count), jnp.float32)
    agreed = jnp.zeros((n_entries, snap_count), jnp.float32)
    states = None
    consensus = None
    for iteration in range(ITERS):
        shifted = jnp.where(mask, agreed - dual_value, 0.0)
        update = jnp.zeros((areas_total * state_size, snap_count), jnp.float32).at[rows_flat].add(shifted)
        blended = (rhs + PENALTY * update).astype(jnp.bfloat16).reshape(areas_total, state_size, snap_count)
        states = lax.map(solve_area, (ginv, blended)).reshape(areas_total * state_size, snap_count)
        local_part = jnp.where(mask, states[rows_flat] + dual_value, 0.0)
        totals = jax.ops.segment_sum(local_part, var_safe, num_segments=VARS)
        consensus = totals * inverse[:, None]
        agreed = jnp.where(mask, consensus[var_safe], 0.0)
        dual_value = jnp.where(mask, local_part - agreed, 0.0)
    return states, consensus, dual_value
```

```python
import functools

import jax
import jax.numpy as jnp
from jax import lax
from jax.experimental import pallas as pl
from jax.experimental.pallas import tpu as pltpu
from jax.sharding import PartitionSpec as P

SLOT = 4
VAR_DEV = 64
ITERS = 4
PENALTY = 1.0

MESH = pl.DeviceIdType.MESH
F32 = jnp.float32
BF16 = jnp.bfloat16


def mm(a, b):
    return jnp.dot(a, b, preferred_element_type=F32)


def dot_dims(a, b, da, db):
    return lax.dot_general(a, b, (((da,), (db,)), ((), ())), preferred_element_type=F32)


def parts(x):
    high = x.astype(BF16)
    rest = x - high.astype(F32)
    mid = rest.astype(BF16)
    low = (rest - mid.astype(F32)).astype(BF16)
    return high, mid, low


def mm_parts(onehot, x):
    high, mid, low = parts(x)
    return mm(onehot, high) + (mm(onehot, mid) + mm(onehot, low))


def kernel(
    area_n,
    tie_n,
    srow_col,
    srow_lane,
    svar_col,
    g_hbm,
    rhs_hbm,
    states_ref,
    cons_ref,
    dual_ref,
    g_ref,
    rhs_ref,
    pick,
    out_buf,
    in_buf,
    rhs_b,
    y_base,
    g_bb,
    load_sem,
    send_sem,
    recv_sem,
):
    devices = area_n * tie_n
    area_dev, state_size, _ = g_ref.shape
    cap = devices * SLOT
    snap = dual_ref.shape[1]
    me_a, me_t = lax.axis_index("area"), lax.axis_index("tie")
    me = me_a * tie_n + me_t

    blocks = 4 if devices % 4 == 0 else 1
    block = devices // blocks
    me_block, me_in = me // block, lax.rem(me, block)
    upper = 2 * me_block >= blocks
    turned = jnp.where(upper, me_block, blocks - 1 - me_block)

    def peer_of(k):
        peer = lax.rem(me + k, devices)
        return peer, (peer // tie_n, lax.rem(peer, tie_n))

    barrier = pltpu.get_barrier_semaphore()

    @pl.loop(1, devices)
    def _(k):
        _, device = peer_of(k)
        pl.semaphore_signal(barrier, inc=1, device_id=device, device_id_type=MESH)

    def g_load(a):
        return pltpu.make_async_copy(g_hbm.at[a], g_ref.at[a], load_sem.at[0, a])

    def rhs_load(a):
        return pltpu.make_async_copy(rhs_hbm.at[a], rhs_ref.at[a], load_sem.at[1, a])

    for a in range(area_dev):
        g_load(a).start()
        rhs_load(a).start()

    def send(phase, value):
        out_buf[phase] = value.reshape(devices, SLOT, snap)
        in_buf[phase, me] = out_buf[phase, me]

        def post(peer):
            pltpu.make_async_remote_copy(
                src_ref=out_buf.at[phase, peer],
                dst_ref=in_buf.at[phase, me],
                send_sem=send_sem.at[phase],
                recv_sem=recv_sem.at[phase],
                device_id=(peer // tie_n, lax.rem(peer, tie_n)),
                device_id_type=MESH,
            ).start()

        @pl.loop(0, blocks - 1)
        def _(b):
            placed = b + jnp.where(b >= turned, 1, 0)
            base = jnp.where(upper, placed, blocks - 1 - placed) * block
            for i in range(block):
                post(base + lax.rem(me_in + i, block))

        for i in range(1, block):
            post(me_block * block + lax.rem(me_in + i, block))

    def receive(phase):
        span = in_buf.at[phase, pl.ds(0, devices - 1)]
        pltpu.make_async_copy(span, span, recv_sem.at[phase]).wait()
        return in_buf[phase].reshape(cap, snap)

    lane = lax.broadcasted_iota(jnp.int32, (cap, snap), 1)
    member_out = (svar_col[...] == lane).astype(F32)
    pl.semaphore_wait(barrier, devices - 1)
    send(0, member_out)

    rhs_b[...] = jnp.zeros_like(rhs_b)
    y_base[...] = jnp.zeros_like(y_base)
    g_bb[...] = jnp.zeros_like(g_bb)

    @pl.loop(0, area_dev)
    def _(a):
        column = lax.broadcasted_iota(jnp.int32, (cap, state_size), 1) + a * state_size
        chosen = (jnp.broadcast_to(srow_col[:, :1], (cap, state_size)) == column).astype(F32)
        chosen = chosen.astype(BF16)
        line = lax.broadcasted_iota(jnp.int32, (state_size, cap), 0) + a * state_size
        pick[a] = (
            (jnp.broadcast_to(srow_lane[:1, :], (state_size, cap)) == line)
            .astype(F32)
            .astype(BF16)
        )
        rhs_load(a).wait()
        high, mid, low = parts(rhs_ref[a])
        rhs_b[...] += mm(chosen, high) + (mm(chosen, mid) + mm(chosen, low))
        g_load(a).wait()
        rows = mm(chosen, g_ref[a]).astype(BF16)
        y_base[...] += mm(rows, high)
        g_bb[...] += mm(rows, pick[a])

    inner = g_bb[...].astype(BF16)
    own = rhs_b[...]
    first = y_base[...]
    steady = first - mm(inner, own.astype(BF16))

    member = receive(0).astype(BF16)
    same = dot_dims(member, member, 1, 1)
    share = 1.0 / jnp.maximum(jnp.sum(same, axis=1, keepdims=True), 1.0)
    same = same.astype(BF16)
    dual = jnp.zeros((cap, snap), F32)
    update = jnp.zeros((cap, snap), F32)
    for it in range(ITERS):
        if it == 0:
            local = first
        else:
            blended = (own + PENALTY * update).astype(BF16)
            local = steady + mm(inner, blended) + dual
        send(1 + 2 * it, local)
        if it == ITERS - 1:
            moved = parts(update)

            @pl.loop(0, area_dev)
            def _(a):
                scattered = mm(pick[a], moved[0]) + (mm(pick[a], moved[1]) + mm(pick[a], moved[2]))
                mixed = (rhs_ref[a] + PENALTY * scattered).astype(BF16)
                states_ref[a] = mm(g_ref[a], mixed)

        incoming = receive(1 + 2 * it)
        send(2 + 2 * it, mm_parts(same, incoming) * share)
        if it == ITERS - 1:
            high, mid, low = parts(incoming)
            totals = dot_dims(member, high, 0, 0) + (
                dot_dims(member, mid, 0, 0) + dot_dims(member, low, 0, 0)
            )
            counts = dot_dims(member, jnp.ones((cap, snap), BF16), 0, 0)
            consensus = totals * (1.0 / jnp.maximum(counts, 1.0))
            cons_ref[...] = consensus[: cons_ref.shape[0]]
        agreed = receive(2 + 2 * it)
        dual = local - agreed
        update = agreed - dual
    dual_ref[...] = dual

    for phase in range(1 + 2 * ITERS):
        span = out_buf.at[phase, pl.ds(0, devices - 1)]
        pltpu.make_async_copy(span, span, send_sem.at[phase]).wait()


def on_device(ginv, rhs, bnd_row, bnd_var):
    area_dev, state_size, _ = ginv.shape
    snap = rhs.shape[1]
    bound_size = bnd_row.shape[1]
    entries = area_dev * bound_size
    area_n = lax.axis_size("area")
    tie_n = lax.axis_size("tie")
    devices = area_n * tie_n
    cap = devices * SLOT
    row_flat = bnd_row.reshape(entries)
    var_flat = bnd_var.reshape(entries)
    active = row_flat >= 0
    order = jnp.arange(entries, dtype=jnp.int32)
    state_row = (order // bound_size) * state_size + row_flat
    owners = jnp.where(active, var_flat // VAR_DEV, devices)
    owned = owners[:, None] == jnp.arange(devices, dtype=jnp.int32)[None, :]
    earlier = (order[:, None] > order[None, :]).astype(BF16)
    before = mm(earlier, owned.astype(BF16))
    placed = jnp.sum(jnp.where(owned, before, 0.0), axis=1).astype(jnp.int32)
    slot = jnp.where(active, owners * SLOT + placed, -1)
    slots = jnp.arange(cap, dtype=jnp.int32)
    held = slots[:, None] == slot[None, :]
    srow = jnp.sum(jnp.where(held, (state_row + 1)[None, :], 0), axis=1) - 1
    svar = jnp.sum(jnp.where(held, (var_flat % VAR_DEV + 1)[None, :], 0), axis=1) - 1
    phases = 1 + 2 * ITERS
    vmem = pl.BlockSpec(memory_space=pltpu.VMEM)
    hbm = pl.BlockSpec(memory_space=pl.ANY)
    states, consensus, dual = pl.pallas_call(
        functools.partial(kernel, area_n, tie_n),
        out_shape=(
            jax.ShapeDtypeStruct((area_dev, state_size, snap), F32),
            jax.ShapeDtypeStruct((VAR_DEV, snap), F32),
            jax.ShapeDtypeStruct((cap, snap), F32),
        ),
        in_specs=[vmem, vmem, vmem, hbm, hbm],
        out_specs=(vmem, vmem, vmem),
        scratch_shapes=[
            pltpu.VMEM(ginv.shape, BF16),
            pltpu.VMEM((area_dev, state_size, snap), F32),
            pltpu.VMEM((area_dev, state_size, cap), BF16),
            pltpu.VMEM((phases, devices, SLOT, snap), F32),
            pltpu.VMEM((phases, devices, SLOT, snap), F32),
            pltpu.VMEM((cap, snap), F32),
            pltpu.VMEM((cap, snap), F32),
            pltpu.VMEM((cap, cap), F32),
            pltpu.SemaphoreType.DMA((2, area_dev)),
            pltpu.SemaphoreType.DMA((phases,)),
            pltpu.SemaphoreType.DMA((phases,)),
        ],
        compiler_params=pltpu.CompilerParams(
            collective_id=0, has_side_effects=True, vmem_limit_bytes=48 * 1024 * 1024
        ),
        name="admm",
    )(
        jnp.broadcast_to(srow[:, None], (cap, snap)),
        jnp.broadcast_to(srow[None, :], (8, cap)),
        jnp.broadcast_to(svar[:, None], (cap, snap)),
        ginv,
        rhs.reshape(area_dev, state_size, snap),
    )
    spread = (slot[:, None] == slots[None, :]).astype(F32)
    dual = jnp.dot(spread, dual, precision=lax.Precision.HIGHEST)
    return (states.reshape(area_dev * state_size, snap), consensus, dual)


def split(x):
    high = x.astype(BF16)
    return high, (x - high.astype(F32)).astype(BF16)


def column_kernel(
    ny,
    area_n,
    tie_n,
    row_hbm,
    var_hbm,
    g_hbm,
    rhs_hbm,
    states_ref,
    cons_ref,
    dual_ref,
    row_ref,
    var_ref,
    g_ref,
    rhs_ref,
    srow_col,
    srow_lane,
    hold_t,
    weights,
    g_cols,
    own_ref,
    first_ref,
    k_ref,
    sv_out,
    sv_in,
    x_out,
    x_in,
    u_out,
    u_in,
    f_out,
    f_in,
    k_buf,
    k16,
    same16,
    var16,
    share_ref,
    count_ref,
    lhs_ref,
    res_ref,
    load_sem,
    index_sem,
    barrier_done,
    send_sem,
    recv_sem,
    k_send,
    k_recv,
    k_pair,
):
    del barrier_done
    D = area_n * tie_n
    area_dev, state_size, _ = g_ref.shape
    bound = row_ref.shape[1]
    cap = D * SLOT
    snap = rhs_ref.shape[2]
    cols = snap // D
    nz = area_n // ny
    var_dev = cons_ref.shape[0]
    me_a, me_t = lax.axis_index("area"), lax.axis_index("tie")
    me = me_a * tie_n + me_t
    z, y, x, c = me_a // ny, lax.rem(me_a, ny), me_t // 2, lax.rem(me_t, 2)

    def place(px, py, pz, pc):
        return pz * ny + py, px * 2 + pc

    def flat(px, py, pz, pc):
        return (pz * ny + py) * tie_n + px * 2 + pc

    barrier = pltpu.get_barrier_semaphore()

    @pl.loop(1, D)
    def _(k):
        peer = lax.rem(me + k, D)
        pl.semaphore_signal(
            barrier, inc=1, device_id=(peer // tie_n, lax.rem(peer, tie_n)), device_id_type=MESH
        )

    def g_load(a):
        return pltpu.make_async_copy(g_hbm.at[a], g_ref.at[a], load_sem.at[0, a])

    def rhs_load(a):
        return pltpu.make_async_copy(rhs_hbm.at[a], rhs_ref.at[a], load_sem.at[1, a])

    row_load = pltpu.make_async_copy(row_hbm, row_ref, index_sem.at[0])
    var_load = pltpu.make_async_copy(var_hbm, var_ref, index_sem.at[1])
    row_load.start()
    var_load.start()
    for a in range(area_dev):
        rhs_load(a).start()
        g_load(a).start()

    def exchange(out_buf, in_buf, phase):
        in_buf[me] = out_buf[me]

        @pl.loop(1, D)
        def _(k):
            peer = lax.rem(me + k, D)
            pltpu.make_async_remote_copy(
                src_ref=out_buf.at[peer],
                dst_ref=in_buf.at[me],
                send_sem=send_sem.at[phase],
                recv_sem=recv_sem.at[phase],
                device_id=(peer // tie_n, lax.rem(peer, tie_n)),
                device_id_type=MESH,
            ).start()

    def arrived(in_buf, phase):
        span = in_buf.at[pl.ds(0, D - 1)]
        pltpu.make_async_copy(span, span, recv_sem.at[phase]).wait()

    def sent(out_buf, phase):
        span = out_buf.at[pl.ds(0, D - 1)]
        pltpu.make_async_copy(span, span, send_sem.at[phase]).wait()

    row_load.wait()
    var_load.wait()
    rows = row_ref[...]
    variables = var_ref[...]
    owner_line = lax.broadcasted_iota(jnp.int32, (D, bound), 0)
    earlier = (
        lax.broadcasted_iota(jnp.int32, (bound, bound), 0)
        < lax.broadcasted_iota(jnp.int32, (bound, bound), 1)
    )
    earlier = earlier.astype(F32).astype(BF16)
    slot_line = lax.broadcasted_iota(jnp.int32, (cap, bound), 0)
    slot_lane = lax.broadcasted_iota(jnp.int32, (bound, cap), 1)
    carry = jnp.zeros((D, 1), F32)
    sv_col = jnp.zeros((cap, bound), F32)
    slot_rows = []
    for a in range(area_dev):
        row, var = rows[a : a + 1], variables[a : a + 1]
        live = row >= 0
        owner = jnp.where(live, var // var_dev, D)
        owned = (jnp.broadcast_to(owner, (D, bound)) == owner_line).astype(F32)
        before = mm(owned.astype(BF16), earlier) + carry
        carry = carry + jnp.sum(owned, axis=1, keepdims=True)
        rank = jnp.sum(owned * before, axis=0, keepdims=True)
        slot = jnp.where(live, rank.astype(jnp.int32) * D + owner, -1)
        slot_rows.append(slot)
        held = jnp.broadcast_to(slot, (cap, bound)) == slot_line
        srow = jnp.sum(
            jnp.where(held, jnp.broadcast_to(row + 1, (cap, bound)), 0).astype(F32),
            axis=1,
            keepdims=True,
        )
        srow_col[a] = jnp.broadcast_to(srow, (cap, bound)) - 1.0
        sv_col = sv_col + jnp.where(
            held, jnp.broadcast_to(lax.rem(var, var_dev) + 1, (cap, bound)), 0
        ).astype(F32)
    sv_wide = jnp.broadcast_to(jnp.sum(sv_col, axis=1, keepdims=True), (cap, bound)) - 1.0
    sv_row = sv_wide.T[:1]
    for a in range(area_dev):
        srow_lane[a] = srow_col[a].T[:8]
    slot_all = jnp.concatenate(slot_rows + [slot_rows[0]] * (8 - area_dev), axis=0).astype(F32)
    slot_cols = jnp.concatenate([slot_all] * (bound // 8), axis=0).T
    for a in range(area_dev):
        column = jnp.broadcast_to(slot_cols[:, a : a + 1], (bound, cap))
        hold_t[a] = (column == slot_lane.astype(F32)).astype(F32).astype(BF16)
    sv_out[...] = jnp.broadcast_to(sv_row.reshape(1, 1, cap), (D, 1, cap))

    pl.semaphore_wait(barrier, D - 1)
    exchange(sv_out, sv_in, 0)

    own_ref[...] = jnp.zeros_like(own_ref)
    first_ref[...] = jnp.zeros_like(first_ref)
    k_ref[...] = jnp.zeros_like(k_ref)

    @pl.loop(0, area_dev)
    def _(a):
        column = lax.broadcasted_iota(jnp.int32, (cap, state_size), 1).astype(F32)
        chosen = jnp.broadcast_to(srow_col[a][:, :1], (cap, state_size)) == column
        chosen = chosen.astype(F32).astype(BF16)
        line = lax.broadcasted_iota(jnp.int32, (state_size, cap), 0).astype(F32)
        pick = jnp.broadcast_to(srow_lane[a][:1], (state_size, cap)) == line
        weights[:, snap:] = pick.astype(F32).astype(BF16)
        rhs_load(a).wait()
        high, mid = split(rhs_ref[a])
        weights[:, :snap] = high
        own_ref[...] += mm(chosen, high) + mm(chosen, mid)
        g_load(a).wait()
        both = mm(g_ref[a], weights[...])
        base = both[:, :snap]
        columns = both[:, snap:].astype(BF16)
        states_ref[a] = base
        g_cols[a] = columns
        high, mid = split(base)
        first_ref[...] += mm(chosen, high) + mm(chosen, mid)
        k_ref[...] += mm(chosen, columns)

    own = own_ref[...]
    k_buf[me] = k_ref[...].T

    total = [0, 0]

    def block(b, part):
        half = cap // 2
        return k_buf.at[b] if part is None else k_buf.at[b, pl.ds(part * half, half)]

    def forward(b, part, device, sem):
        ref = block(b, part)
        total[0] += 2 if part is None else 1
        pltpu.make_async_remote_copy(
            src_ref=ref,
            dst_ref=ref,
            send_sem=k_send,
            recv_sem=sem,
            device_id=device,
            device_id_type=MESH,
        ).start()

    def landed(b, part, sem):
        ref = block(b, part)
        pltpu.make_async_copy(ref, ref, sem).wait()

    x_next, y_next, pair = place(1 - x, y, z, c), place(x, 1 - y, z, c), place(x, y, z, 1 - c)
    heights = [lax.rem(z + k, nz) for k in range(nz)]

    x_out[:, pl.ds(0, cols), :] = first_ref[...].T.reshape(D, cols, cap)
    x_out[:, pl.ds(cols, cols), :] = own.T.reshape(D, cols, cap)
    forward(me, None, x_next, k_recv.at[me, 0])
    forward(me, None, y_next, k_recv.at[me, 0])
    for k in range(1, nz):
        forward(me, None, place(x, y, heights[k], c), k_recv.at[me, 0])
    exchange(x_out, x_in, 1)
    forward(me, None, pair, k_pair.at[me])

    lane_block = lax.broadcasted_iota(jnp.int32, (D, cap), 1) // D

    def shuffle(p):
        turned = p.T
        rolled = [turned] + [pltpu.roll(turned, k * D, 1) for k in range(1, SLOT)]
        parts_out = []
        for i in range(cols):
            piece = rolled[(0 - i) % SLOT][:D]
            for s in range(1, SLOT):
                piece = jnp.where(
                    lane_block == s, rolled[(s - i) % SLOT][s * D : (s + 1) * D], piece
                )
            parts_out.append(piece)
        return jnp.concatenate(parts_out, axis=0)

    arrived(sv_in, 0)
    sv = sv_in[...].reshape(D, cap)
    sv_q = shuffle(jnp.concatenate([sv] * cols, axis=0))
    sv_t = sv_q.T
    var_lane = lax.broadcasted_iota(jnp.int32, (cap, cap), 1).astype(F32)
    for o in range(D):
        column = jnp.broadcast_to(sv_t[:, o : o + 1], (cap, cap))
        line = jnp.broadcast_to(sv_q[o : o + 1], (cap, cap))
        equal = ((column == line) & (line >= 0.0)).astype(F32)
        hit = (column == var_lane).astype(F32)
        same16[o] = equal.astype(BF16)
        var16[o] = hit.astype(BF16)
        share_ref[pl.ds(o, 1)] = 1.0 / jnp.maximum(jnp.sum(equal, axis=0, keepdims=True), 1.0)
        count_ref[pl.ds(o, 1)] = 1.0 / jnp.maximum(jnp.sum(hit, axis=0, keepdims=True), 1.0)

    for k in range(1, nz):
        b = flat(x, y, heights[k], c)
        landed(b, None, k_recv.at[b, 0])
        forward(b, None, x_next, k_recv.at[b, 0])
        forward(b, None, y_next, k_recv.at[b, 0])
        forward(b, None, pair, k_pair.at[b])

    def put(ref, base, value):
        for i in range(cols):
            ref[:, base + i, :] = value[i * D : (i + 1) * D]

    def get(ref, base):
        return jnp.concatenate([ref[:, base + i, :] for i in range(cols)], axis=0)

    share = jnp.concatenate([share_ref[...]] * cols, axis=0)

    def average(local, last):
        q = shuffle(local)
        high = q.astype(BF16).astype(F32)
        put(lhs_ref, 0, high)
        put(lhs_ref, cols, q - high)
        for o in range(D):
            left = lhs_ref[o].astype(BF16)
            res_ref[o] = mm(left, same16[o])
            if last:
                both = mm(left, var16[o])
                f_out[o, pl.ds(cols, cols)] = (both[:cols] + both[cols:]) * count_ref[pl.ds(o, 1)]
        return shuffle((get(res_ref, 0) + get(res_ref, cols)) * share)

    arrived(x_in, 1)
    first = get(x_in, 0)
    own_p = get(x_in, cols)
    local = first
    agreed = average(local, False)
    dual = local - agreed
    update = agreed - dual

    for k in range(nz):
        bx, by = flat(1 - x, y, heights[k], c), flat(x, 1 - y, heights[k], c)
        landed(bx, None, k_recv.at[bx, 0])
        forward(bx, 0, y_next, k_recv.at[bx, 0])
        forward(bx, None, pair, k_pair.at[bx])
        landed(by, None, k_recv.at[by, 0])
        forward(by, 1, x_next, k_recv.at[by, 1])
        forward(by, None, pair, k_pair.at[by])
    for k in range(nz):
        b = flat(1 - x, 1 - y, heights[k], c)
        landed(b, 0, k_recv.at[b, 0])
        landed(b, 1, k_recv.at[b, 1])
        forward(b, None, pair, k_pair.at[b])
    for px in range(2):
        for py in range(ny):
            for pz in range(nz):
                b = flat(px, py, pz, 1 - c)
                landed(b, None, k_pair.at[b])

    put(lhs_ref, 0, own_p)
    put(lhs_ref, cols, own_p + PENALTY * update)
    for d in range(D):
        k16[d] = k_buf[d].astype(BF16)
        res_ref[d] = mm(lhs_ref[d].astype(BF16), k16[d])
    steady = first - get(res_ref, 0)
    local = steady + get(res_ref, cols) + dual

    for it in range(1, ITERS):
        agreed = average(local, it == ITERS - 1)
        dual = local - agreed
        update = agreed - dual
        if it == ITERS - 1:
            put(f_out, 0, dual)
            exchange(f_out, f_in, 3)
            break
        if it == ITERS - 2:
            put(u_out, 0, update)
            exchange(u_out, u_in, 2)
        put(lhs_ref, 0, own_p + PENALTY * update)
        for d in range(D):
            res_ref[d] = mm(lhs_ref[d].astype(BF16), k16[d])
        local = steady + get(res_ref, 0) + dual

    arrived(u_in, 2)
    final = u_in[...].reshape(snap, cap).T
    moved = (own + PENALTY * final).astype(BF16).astype(F32) - own.astype(BF16).astype(F32)
    high, mid = split(moved)

    @pl.loop(0, area_dev)
    def _(a):
        states_ref[a] += mm(g_cols[a], high) + mm(g_cols[a], mid)

    arrived(f_in, 3)
    dual = f_in[:, pl.ds(0, cols), :].reshape(snap, cap).T
    high, mid = split(dual)
    for a in range(area_dev):
        dual_ref[pl.ds(a * bound, bound)] = mm(hold_t[a], high) + mm(hold_t[a], mid)
    consensus = f_in[:, pl.ds(cols, cols), :].reshape(snap, cap).T
    cons_ref[...] = consensus[:var_dev]

    sent(sv_out, 0)
    sent(x_out, 1)
    sent(u_out, 2)
    sent(f_out, 3)
    whole = k_buf.at[0]
    for _ in range(total[0] // 2):
        pltpu.make_async_copy(whole, whole, k_send).wait()
    if total[0] % 2:
        landed(0, 0, k_send)


def on_device_columns(ginv, rhs, bnd_row, bnd_var):
    area_dev, state_size, _ = ginv.shape
    snap = rhs.shape[1]
    bound = bnd_row.shape[1]
    area_n = lax.axis_size("area")
    tie_n = lax.axis_size("tie")
    D = area_n * tie_n
    cap = D * SLOT
    cols = snap // D
    ny = tie_n // 2
    vmem = pl.BlockSpec(memory_space=pltpu.VMEM)
    hbm = pl.BlockSpec(memory_space=pltpu.HBM)
    V = pltpu.VMEM
    states, consensus, dual = pl.pallas_call(
        functools.partial(column_kernel, ny, area_n, tie_n),
        out_shape=(
            jax.ShapeDtypeStruct((area_dev, state_size, snap), F32),
            jax.ShapeDtypeStruct((VAR_DEV, snap), F32),
            jax.ShapeDtypeStruct((area_dev * bound, snap), F32),
        ),
        in_specs=[hbm] * 4,
        out_specs=(vmem, vmem, vmem),
        scratch_shapes=[
            V((area_dev, bound), jnp.int32),
            V((area_dev, bound), jnp.int32),
            V(ginv.shape, BF16),
            V((area_dev, state_size, snap), F32),
            V((area_dev, cap, bound), F32),
            V((area_dev, 8, cap), F32),
            V((area_dev, bound, cap), BF16),
            V((state_size, snap + cap), BF16),
            V((area_dev, state_size, cap), BF16),
            V((cap, snap), F32),
            V((cap, snap), F32),
            V((cap, cap), F32),
            V((D, 1, cap), F32),
            V((D, 1, cap), F32),
            V((D, 2 * cols, cap), F32),
            V((D, 2 * cols, cap), F32),
            V((D, cols, cap), F32),
            V((D, cols, cap), F32),
            V((D, 2 * cols, cap), F32),
            V((D, 2 * cols, cap), F32),
            V((D, cap, cap), F32),
            V((D, cap, cap), BF16),
            V((D, cap, cap), BF16),
            V((D, cap, cap), BF16),
            V((D, cap), F32),
            V((D, cap), F32),
            V((D, 2 * cols, cap), F32),
            V((D, 2 * cols, cap), F32),
            pltpu.SemaphoreType.DMA((2, area_dev)),
            pltpu.SemaphoreType.DMA((2,)),
            pltpu.SemaphoreType.DMA,
            pltpu.SemaphoreType.DMA((4,)),
            pltpu.SemaphoreType.DMA((4,)),
            pltpu.SemaphoreType.DMA,
            pltpu.SemaphoreType.DMA((D, 2)),
            pltpu.SemaphoreType.DMA((D,)),
        ],
        compiler_params=pltpu.CompilerParams(
            collective_id=0, has_side_effects=True, vmem_limit_bytes=56 * 1024 * 1024
        ),
        name="admm_columns",
    )(bnd_row, bnd_var, ginv, rhs.reshape(area_dev, state_size, snap))
    return (states.reshape(area_dev * state_size, snap), consensus, dual)


def columns_fit(mesh, snap):
    area_n, tie_n = mesh.shape["area"], mesh.shape["tie"]
    cap = area_n * tie_n * SLOT
    return tie_n == 4 and area_n % 2 == 0 and snap == cap == 128


def on_any_device(mesh, ginv, rhs, bnd_row, bnd_var):
    step = on_device_columns if columns_fit(mesh, rhs.shape[1]) else on_device
    return step(ginv, rhs, bnd_row, bnd_var)


def solution(mesh):
    both = ("area", "tie")
    in_specs = (P(both, None, None), P(both, None), P(both, None), P(both, None))
    out_specs = (P(both, None), P(both, None), P(both, None))
    return jax.shard_map(
        functools.partial(on_any_device, mesh), mesh=mesh, in_specs=in_specs, out_specs=out_specs, check_vma=False
    )
```
